256 devices in a mesh: head: 2 (over core), blk: 32 (over z, x), rep: 4 (over y).
Axes of the slice: x: 4, y: 4, z: 8, core: 2. Of those that a mesh axis runs over, the one named last changes fastest.
Arguments:
- queries: bfloat16 [16384, 768], P(('blk', 'rep'), 'head'), may hold values from -400 to 400
- keys: bfloat16 [16384, 256], P(('blk', 'rep'), 'head'), may hold values from -6 to 6
- values: bfloat16 [16384, 256], P(('blk', 'rep'), 'head'), may hold values from -18 to 18
- stretch_order: int32 [128], replicated, may hold values from 0 to 127, each once
- out_weight: bfloat16 [768, 3072], P('head'), may hold values from -0.21875 to 0.21875
Outputs:
- mixed_rows: bfloat16 [16384, 3072], P(('blk', 'rep'), 'head')
- log_sum_exp: float32 [6, 16384], P('head', ('blk', 'rep'))
The draws below stay inside these ranges and needn't reach their ends.
Inputs may be any that keep to these rules, and one draw needn't show every extreme that they name: `stretch_order`: each stretch number appears once.
All inputs are finite; a program needn't handle non-finite values.
Results may differ from the reference program's by a relative error of at most 0.02.
Values may be sent and summed in bfloat16 or wider, within the bound.
A program may use at most 128 MiB of HBM per device.

```python
import math
import jax
import jax.numpy as jnp
from jax import lax

D = 3072
GROUP = 3
DH = 128
KVH_DEV = 1
TOK_DEV = 128
KV_HEADS = 2
QHEADS = 6
NCHUNKS = 128
SEQ = 16384
N_HEAD = 2


def draw_keys(key, part):
    drawn_keys = jnp.clip(jax.random.normal(jax.random.fold_in(key, 3), (SEQ, KV_HEADS * DH), jnp.float32), -6.0, 6.0)
    return drawn_keys.astype(jnp.bfloat16)


def draw_queries(key, part):
    drawn_queries = jnp.clip(2.0 * jax.random.normal(jax.random.fold_in(key, 5), (SEQ, QHEADS * DH), jnp.float32), -12.0, 12.0)
    return drawn_queries.astype(jnp.bfloat16)


def block_scale(stream_key, extent, pieces, least, top_value):
    def one(axis_at, blocks):
        draws = jax.random.uniform(jax.random.fold_in(jax.random.fold_in(stream_key, 6), axis_at), (blocks,), jnp.float32, least / len(pieces), top_value / len(pieces))
        return jnp.repeat(jnp.exp(draws), extent[axis_at] // blocks).reshape((-1,) + (1,) * (len(extent) - axis_at - 1))

    factor_of = one(*pieces[0])
    for cut in pieces[1:]:
        factor_of = factor_of * one(*cut)
    return factor_of


def normal_values(stream_key, extent, scale, limit, cuts=(), kind=jnp.bfloat16):
    loudness = block_scale(stream_key, extent, cuts, -0.22, 0.18) if cuts else 1.0
    array = jax.random.normal(stream_key, extent, jnp.float32) * scale * loudness
    return jnp.minimum(jnp.maximum(array, -limit), limit).astype(kind)


def setup_inputs(seed: int = 0) -> dict:
    splits = jax.random.split(jax.random.key(seed), 6)
    queries = draw_queries(jax.random.fold_in(splits[5], 71), 0)
    keys = draw_keys(jax.random.fold_in(splits[5], 71), 0)
    values = normal_values(splits[2], (SEQ, KV_HEADS * DH), 3.0, 18.0, ((0, 128), (1, 2)))
    stretch_order = jax.random.permutation(splits[3], NCHUNKS).astype(jnp.int32)
    out_weight = normal_values(splits[4], (QHEADS * DH, D), (QHEADS * DH) ** -0.5, 0.21875, ((0, 2),))
    return dict(queries=queries, keys=keys, values=values, stretch_order=stretch_order, out_weight=out_weight)


def reference(queries, keys, values, stretch_order, out_weight):
    seq_len = queries.shape[0]
    row_ids = jnp.arange(seq_len, dtype=jnp.int32)
    positions = stretch_order[row_ids // TOK_DEV].astype(jnp.int32) * TOK_DEV + row_ids % TOK_DEV
    query_heads = queries.astype(jnp.float32).reshape(seq_len, QHEADS, DH).transpose(1, 0, 2)
    key_heads = keys.astype(jnp.float32).reshape(seq_len, KV_HEADS, DH).transpose(1, 0, 2)
    value_heads = values.astype(jnp.float32).reshape(seq_len, KV_HEADS, DH).transpose(1, 0, 2)
    block_len = math.gcd(seq_len, 1024)
    block_count = seq_len // block_len
    factor = DH ** (-0.5)

    def one_block(flat_index):
        head_index = flat_index // block_count
        block_index = flat_index % block_count
        group_index = head_index // GROUP
        query_head = lax.dynamic_index_in_dim(query_heads, head_index, 0, keepdims=False)
        query_block = lax.dynamic_slice_in_dim(query_head, block_index * block_len, block_len, 0)
        key_head = lax.dynamic_index_in_dim(key_heads, group_index, 0, keepdims=False)
        value_head = lax.dynamic_index_in_dim(value_heads, group_index, 0, keepdims=False)
        query_pos = lax.dynamic_slice_in_dim(positions, block_index * block_len, block_len, 0)
        scores = jnp.dot(query_block, key_head.T, precision=lax.Precision.HIGHEST) * factor
        allowed = positions[None, :] <= query_pos[:, None]
        masked = jnp.where(allowed, scores, -jnp.inf)
        row_top = jnp.max(masked, axis=1)
        expanded = jnp.where(allowed, jnp.exp(scores - row_top[:, None]), 0.0)
        totals = jnp.sum(expanded, axis=1)
        weights = lax.optimization_barrier(expanded.astype(jnp.bfloat16)).astype(jnp.float32)
        attended = jnp.dot(weights, value_head, precision=lax.Precision.HIGHEST) / totals[:, None]
        return (attended.astype(jnp.bfloat16), row_top + jnp.log(totals))
    outputs, sums = lax.map(one_block, jnp.arange(QHEADS * block_count, dtype=jnp.int32))
    attended = outputs.reshape(QHEADS, seq_len, DH).transpose(1, 0, 2).reshape(seq_len, QHEADS * DH)
    log_sum_exp = sums.reshape(QHEADS, seq_len)
    width = KVH_DEV * GROUP * DH
    mixed = jnp.zeros((seq_len, out_weight.shape[1]), jnp.float32)
    for rank in range(N_HEAD):
        partial_value = jnp.dot(attended[:, rank * width:(rank + 1) * width].astype(jnp.float32), out_weight[rank * width:(rank + 1) * width].astype(jnp.float32), precision=lax.Precision.HIGHEST)
        mixed = mixed + lax.optimization_barrier(partial_value.astype(jnp.bfloat16)).astype(jnp.float32)
    return (mixed.astype(jnp.bfloat16), log_sum_exp)
```

```python
import functools
import heapq
import math

import jax
import jax.numpy as jnp
from jax import lax
from jax.experimental import pallas as pl
from jax.experimental.pallas import tpu as pltpu
from jax.sharding import Mesh
from jax.sharding import PartitionSpec as P

GROUP = 3
DH = 128
BLK_REP = ("blk_0", "blk_1", "rep")
AXIS = {"z": "blk_0", "x": "blk_1", "y": "rep"}
NEG = -1e30
LOG2E = 1.0 / math.log(2.0)
LN2 = math.log(2.0)
WHOLE, FIRST, SECOND = 0, 1, 2
SLOT_DY = (0, 1, 3, 2)


def ring_sends(offset, n):
    half, out = n // 2, []
    if offset == 0 or offset < half:
        new = offset + 1
        if new <= half:
            out.append((1, new, WHOLE if new < half else FIRST))
    if offset == 0 or offset > half:
        new = (offset or n) - 1
        if new >= half:
            out.append((-1, new, WHOLE if new > half else SECOND))
    return out


def parts_of(key, nz, nx, ny):
    if key[0] == "q":
        return 2 if key[1] == ny // 2 else 1
    _, half, dz, dx = key
    if half == 0:
        return 2 if (dz == 0 and dx == nx // 2) or dz == nz // 2 else 1
    return 2 if (dx == 0 and dz == nz // 2) or dx == nx // 2 else 1


def sends_of(key, nz, nx, ny):
    if key[0] == "q":
        return [("y", s, ("q", new), p) for s, new, p in ring_sends(key[1], ny)]
    _, half, dz, dx = key
    along_z = [("z", s, ("kv", half, new, dx), p) for s, new, p in ring_sends(dz, nz)]
    along_x = [("x", s, ("kv", half, dz, new), p) for s, new, p in ring_sends(dx, nx)]
    if half == 0:
        return (along_x if dz == 0 else []) + along_z
    return (along_z if dx == 0 else []) + along_x


def planes_in_order(nz):
    order = [0]
    for d in range(1, nz // 2):
        order += [d, nz - d]
    return order + [nz // 2]


def compute_units(nz, nx):
    planes = planes_in_order(nz)
    pieces = lambda p: [("kv", h, p, dx) for h in (0, 1) for dx in range(nx)]
    need_q = [[("q", SLOT_DY[0]), ("q", SLOT_DY[1])], [("q", SLOT_DY[2]), ("q", SLOT_DY[3])]]
    units = [(("first", r, 0), pieces(0) + need_q[r], 0.6) for r in (0, 1)]
    for c in range((nz - 2) // 2):
        needs = pieces(planes[1 + 2 * c]) + pieces(planes[2 + 2 * c])
        units += [(("main", r, c), needs + need_q[r], 1.0) for r in (0, 1)]
    units += [(("last", slot, 0), pieces(nz // 2), 0.35) for slot in (3, 1, 2, 0)]
    return units


def plan(nz, nx, ny, latency=2.0, rate=46500.0, issue=0.02):
    units = compute_units(nz, nx)
    busy, coming, took, done, steps, now = {}, [], {}, set(), [], 0.0

    def complete(key):
        done.add(key)
        size = 98304 if key[0] == "q" else 32768
        for axis, sign, new, part in sends_of(key, nz, nx, ny):
            nbytes = size if part == WHOLE else size // 2
            end = max(busy.get((axis, sign), 0.0), now) + nbytes / rate
            busy[axis, sign] = end
            heapq.heappush(coming, (end + latency, new, part))

    for key in (("kv", 0, 0, 0), ("kv", 1, 0, 0), ("q", 0)):
        complete(key)
    while coming or units:
        if coming and coming[0][0] <= now:
            _, key, part = heapq.heappop(coming)
            now += issue
            steps.append(("take", key, part))
            took[key] = took.get(key, 0) + 1
            if took[key] == parts_of(key, nz, nx, ny):
                complete(key)
            continue
        ready, seen = [], set()
        for u in units:
            rows = u[0][1] // 2 if u[0][0] == "last" else u[0][1]
            if rows not in seen and all(d in done for d in u[1]):
                ready.append(u)
            seen.add(rows)
        if ready:
            units.remove(ready[0])
            now += ready[0][2]
            steps.append(ready[0][0])
            continue
        now = coming[0][0]
    return steps


def kernel(
    sizes,
    q_hbm, k_hbm, v_hbm, order_ref, w_hbm,
    out_ref, lse_ref,
    q_buf, kv, m_buf, acc, w_buf, own_o, own_st, o_send, st_send, o_recv, st_recv, relay,
    p_send, p_recv,
    load_sem, kv_recv, q_recv, kv_send, q_send, o_send_sem, st_send_sem, o_recv_sem, st_recv_sem,
    relay_sem, relay_send, p_sem,
):
    nz, nx, ny = sizes
    tok = k_hbm.shape[0]
    hb = tok // 2
    head = lax.axis_index("head")
    pos = {a: lax.axis_index(AXIS[a]) for a in "zxy"}
    size = {"z": nz, "x": nx, "y": ny}

    def at(axis, delta):
        n = size[axis]
        return lax.rem(pos[axis] + (delta + n), n)

    def peer(axis, delta):
        return {AXIS[axis]: at(axis, delta)}

    loads = []
    for g in range(GROUP):
        loads.append((q_hbm.at[:, g * DH:(g + 1) * DH], q_buf.at[0, g]))
    for h in (0, 1):
        loads.append((k_hbm.at[h * hb:(h + 1) * hb], kv.at[0, h, 0]))
        loads.append((v_hbm.at[h * hb:(h + 1) * hb], kv.at[0, h, 1]))
    for c in (0, 1):
        width = out_ref.shape[1]
        loads.append((w_hbm.at[:, c * width:(c + 1) * width], w_buf.at[c]))
    loads = [pltpu.make_async_copy(s, d, load_sem.at[i]) for i, (s, d) in enumerate(loads)]
    for copy in loads[3:7] + loads[:3]:
        copy.start()

    barrier = pltpu.get_barrier_semaphore()
    peers = [peer(a, s) for a in "zxy" for s in (1, -1)] + [peer("y", 2), {"head": 1 - head}]
    for p in peers:
        pl.semaphore_signal(barrier, inc=1, device_id=p, device_id_type=pl.DeviceIdType.MESH)
    for copy in loads[3:7]:
        copy.wait()
    pl.semaphore_wait(barrier, len(peers))

    planes = planes_in_order(nz)
    place = {p: i for i, p in enumerate(planes)}

    def view(key, part):
        if key[0] == "q":
            ref = q_buf.at[SLOT_DY.index(key[1])]
            if part == WHOLE:
                return ref
            return ref.at[:, (part - 1) * hb:part * hb]
        _, h, dz, dx = key
        ref = kv.at[place[dz] * nx + dx, h]
        return ref if part == WHOLE else ref.at[part - 1]

    def arrival_sem(key, part):
        second = 1 if part == SECOND else 0
        if key[0] == "q":
            return q_recv.at[2 * key[1] + second]
        _, h, dz, dx = key
        return kv_recv.at[((h * nz + dz) * nx + dx) * 2 + second]

    def send_on(key):
        for axis, sign, new, part in sends_of(key, nz, nx, ny):
            pltpu.make_async_remote_copy(
                src_ref=view(key, part),
                dst_ref=view(new, part),
                send_sem=q_send if key[0] == "q" else kv_send,
                recv_sem=arrival_sem(new, part),
                device_id=peer(axis, sign),
                device_id_type=pl.DeviceIdType.MESH,
            ).start()

    taken = {}

    def take(key, part):
        ref = view(key, part)
        pltpu.make_async_copy(ref, ref, arrival_sem(key, part)).wait()
        taken[key] = taken.get(key, 0) + 1
        if taken[key] == parts_of(key, nz, nx, ny):
            send_on(key)

    factor = DH ** (-0.5) * LOG2E

    def query_place(slot):
        return order_ref[(pos["z"] * nx + pos["x"]) * ny + at("y", -SLOT_DY[slot])]

    def key_place(plane, dx):
        return order_ref[(at("z", -plane) * nx + at("x", -dx)) * ny + pos["y"]]

    def bias_row(slot, chunk):
        mine = query_place(slot)
        parts = []
        for plane in chunk:
            for dx in range(nx):
                b = jnp.where(key_place(plane, dx) > mine, NEG, 0.0).astype(jnp.float32)
                parts.append(jnp.full((1, tok), b, jnp.float32))
        return jnp.concatenate(parts, axis=1)

    def rows_of(which, chunk):
        rows = []
        for plane in chunk:
            for dx in range(nx):
                for h in (0, 1):
                    rows.append(kv[place[plane] * nx + dx, h, which])
        return jnp.concatenate(rows, axis=0)

    def attend(slots, chunk, first):
        key_rows = rows_of(0, chunk)
        value_rows = rows_of(1, chunk)
        value_rows = jnp.concatenate([value_rows, jnp.ones_like(value_rows)], axis=1)
        for slot in slots:
            bias = bias_row(slot, chunk)
            if first and slot == 0:
                r = lax.broadcasted_iota(jnp.int32, (tok, tok), 0)
                c = lax.broadcasted_iota(jnp.int32, (tok, tok), 1)
                corner = jnp.where(c <= r, 0.0, NEG).astype(jnp.float32)
                rest = jnp.broadcast_to(bias[:, tok:], (tok, bias.shape[1] - tok))
                bias = jnp.concatenate([corner, rest], axis=1)
            for g in range(GROUP):
                scores = lax.dot_general(
                    q_buf[slot, g], key_rows, (((1,), (1,)), ((), ())),
                    preferred_element_type=jnp.float32,
                )
                scores = scores * factor + bias
                top = jnp.max(scores, axis=1, keepdims=True)
                if not first:
                    old = m_buf[slot, g]
                    new = jnp.maximum(old, top)
                    shrink = jnp.exp2(old - new)
                    top = new[:, :1]
                else:
                    new = jnp.broadcast_to(top, (tok, DH))
                weights = jnp.exp2(scores - top).astype(jnp.bfloat16)
                both = jnp.dot(weights, value_rows, preferred_element_type=jnp.float32)
                if not first:
                    both = both + acc[slot, g] * jnp.concatenate([shrink, shrink], axis=1)
                m_buf[slot, g] = new
                acc[slot, g] = both

    def finish(slot):
        row = lax.broadcasted_iota(jnp.int32, (8, tok), 0)
        stats = None
        for g in range(GROUP):
            both = acc[slot, g]
            total = both[:, DH:]
            o = both[:, :DH] / total
            flat = jnp.transpose(m_buf[slot, g] + jnp.log(total) * LOG2E)[:8]
            stats = flat if g == 0 else jnp.where(row < g, stats, flat)
            if slot == 0:
                own_o[g] = o
            else:
                o_send[slot, g] = o.astype(jnp.bfloat16)
        if slot == 0:
            own_st[...] = stats
        else:
            st_send[slot] = stats

    def remote(src, dst, send, recv, to):
        return pltpu.make_async_remote_copy(
            src_ref=src, dst_ref=dst, send_sem=send, recv_sem=recv,
            device_id=to, device_id_type=pl.DeviceIdType.MESH,
        )

    def back(slot):
        dy = SLOT_DY[slot]
        st = remote(st_send.at[slot], st_recv.at[slot], st_send_sem.at[slot], st_recv_sem.at[slot],
                    peer("y", -dy if dy < ny - 1 else 1))
        if dy == ny // 2:
            return [
                remote(o_send.at[slot, :, :hb], relay.at[0], o_send_sem.at[0], relay_sem.at[0],
                       peer("y", 1)),
                remote(o_send.at[slot, :, hb:], relay.at[1], o_send_sem.at[3], relay_sem.at[1],
                       peer("y", -1)),
                st,
            ]
        return [
            remote(o_send.at[slot], o_recv.at[slot], o_send_sem.at[slot], o_recv_sem.at[slot],
                   peer("y", -1 if dy == 1 else 1)),
            st,
        ]

    send_on(("kv", 1, 0, 0))
    send_on(("kv", 0, 0, 0))
    for copy in loads[:3]:
        copy.wait()
    send_on(("q", 0))
    for copy in loads[7:]:
        copy.start()

    sent = []
    for step in plan(nz, nx, ny):
        if step[0] == "take":
            take(*step[1:])
            continue
        kind, which, c = step
        if kind == "first":
            attend((0, 1) if which == 0 else (2, 3), (0,), True)
        elif kind == "main":
            attend((0, 1) if which == 0 else (2, 3), planes[1 + 2 * c:3 + 2 * c], False)
        else:
            attend((which,), (nz // 2,), False)
            finish(which)
            if which:
                copies = back(which)
                for copy in copies:
                    copy.start()
                sent += copies

    far = SLOT_DY.index(ny // 2)
    onward = [
        remote(relay.at[0], o_recv.at[far, :, :hb], relay_send.at[0], o_recv_sem.at[0], peer("y", 1)),
        remote(relay.at[1], o_recv.at[far, :, hb:], relay_send.at[1], o_recv_sem.at[3], peer("y", -1)),
    ]
    for i, copy in enumerate(onward):
        pltpu.make_async_copy(relay.at[i], relay.at[i], relay_sem.at[i]).wait()
        copy.start()

    for copy in loads[7:]:
        copy.wait()
    for slot in (1, 2, 3):
        pltpu.make_async_copy(st_recv.at[slot], st_recv.at[slot], st_recv_sem.at[slot]).wait()
    logs = [own_st[...]] + [st_recv[slot] for slot in (1, 2, 3)]
    top = functools.reduce(jnp.maximum, logs)
    parts = [jnp.exp2(a - top) for a in logs]
    total = functools.reduce(jnp.add, parts)
    lse_ref[...] = (top * LN2 + jnp.log(total))[:GROUP]
    shares = [p / total for p in parts]
    shares = jnp.concatenate(shares + [jnp.zeros((DH - 32, tok), jnp.float32)], axis=0)
    shares = jnp.transpose(shares)

    for slot in (1, 2):
        pltpu.make_async_copy(o_recv.at[slot], o_recv.at[slot], o_recv_sem.at[slot]).wait()
    for copy in onward:
        copy.wait_recv()
    attended = []
    for g in range(GROUP):
        o = own_o[g] * shares[:, g:g + 1]
        for slot in (1, 2, 3):
            o = o + o_recv[slot, g].astype(jnp.float32) * shares[:, 8 * slot + g:8 * slot + g + 1]
        attended.append(o.astype(jnp.bfloat16))
    attended = jnp.concatenate(attended, axis=1)

    width = out_ref.shape[1]
    tile = width // 3
    for j in range(0, width, tile):
        p = jnp.dot(attended, w_buf[1 - head, :, j:j + tile], preferred_element_type=jnp.float32)
        p_send[:, j:j + tile] = p.astype(jnp.bfloat16)
    swap = remote(p_send, p_recv, p_sem.at[0], p_sem.at[1], {"head": 1 - head})
    swap.start()
    for j in range(0, width, tile):
        p = jnp.dot(attended, w_buf[head, :, j:j + tile], preferred_element_type=jnp.float32)
        out_ref[:, j:j + tile] = p.astype(jnp.bfloat16)
    swap.wait_recv()
    out_ref[...] = (out_ref[...].astype(jnp.float32) + p_recv[...].astype(jnp.float32)).astype(
        jnp.bfloat16
    )

    pltpu.make_async_copy(kv.at[1:], kv.at[1:], kv_send).wait()
    pltpu.make_async_copy(q_buf.at[1:], q_buf.at[1:], q_send).wait()
    for copy in sent + onward + [swap]:
        copy.wait_send()


def body(sizes, queries, keys, values, stretch_order, out_weight):
    nz, nx, ny = sizes
    tok = queries.shape[0]
    width = out_weight.shape[1] // 2
    bf, f32 = jnp.bfloat16, jnp.float32
    hbm = pl.BlockSpec(memory_space=pl.ANY)
    dma = pltpu.SemaphoreType.DMA
    call = pl.pallas_call(
        functools.partial(kernel, sizes),
        name="attend_and_project",
        out_shape=(
            jax.ShapeDtypeStruct((tok, width), bf),
            jax.ShapeDtypeStruct((GROUP, tok), f32),
        ),
        in_specs=[hbm, hbm, hbm, pl.BlockSpec(memory_space=pltpu.SMEM), hbm],
        out_specs=(
            pl.BlockSpec(memory_space=pltpu.VMEM),
            pl.BlockSpec(memory_space=pltpu.VMEM),
        ),
        scratch_shapes=[
            pltpu.VMEM((ny, GROUP, tok, DH), bf),
            pltpu.VMEM((nz * nx, 2, 2, tok // 2, DH), bf),
            pltpu.VMEM((ny, GROUP, tok, DH), f32),
            pltpu.VMEM((ny, GROUP, tok, 2 * DH), f32),
            pltpu.VMEM((2, GROUP * DH, width), bf),
            pltpu.VMEM((GROUP, tok, DH), f32),
            pltpu.VMEM((8, tok), f32),
            pltpu.VMEM((ny, GROUP, tok, DH), bf),
            pltpu.VMEM((ny, 8, tok), f32),
            pltpu.VMEM((ny, GROUP, tok, DH), bf),
            pltpu.VMEM((ny, 8, tok), f32),
            pltpu.VMEM((2, GROUP, tok // 2, DH), bf),
            pltpu.VMEM((tok, width), bf),
            pltpu.VMEM((tok, width), bf),
            dma((9,)),
            dma((4 * nz * nx,)),
            dma((2 * ny,)),
            dma,
            dma,
            dma((4,)),
            dma((4,)),
            dma((4,)),
            dma((4,)),
            dma((2,)),
            dma((2,)),
            dma((2,)),
        ],
        compiler_params=pltpu.CompilerParams(
            collective_id=0, has_side_effects=True, vmem_limit_bytes=60 * 1024 * 1024
        ),
    )
    return call(queries, keys, values, stretch_order, out_weight)


def solution(mesh):
    nz, nx, ny = 8, 4, mesh.shape["rep"]
    split = Mesh(
        mesh.devices.reshape(mesh.shape["head"], nz, nx, ny),
        ("head", "blk_0", "blk_1", "rep"),
    )
    in_specs = (P(BLK_REP, "head"), P(BLK_REP, "head"), P(BLK_REP, "head"), P(), P("head", None))
    out_specs = (P(BLK_REP, "head"), P("head", BLK_REP))
    return jax.shard_map(
        functools.partial(body, (nz, nx, ny)),
        mesh=split, in_specs=in_specs, out_specs=out_specs, check_vma=False,
    )
```

```python
import functools
import heapq
import math

import jax
import jax.numpy as jnp
from jax import lax
from jax.experimental import pallas as pl
from jax.experimental.pallas import tpu as pltpu
from jax.sharding import Mesh
from jax.sharding import PartitionSpec as P

GROUP = 3
DH = 128
BLK_REP = ("blk_0", "blk_1", "rep")
AXIS = {"z": "blk_0", "x": "blk_1", "y": "rep"}
NEG = -1e30
LOG2E = 1.0 / math.log(2.0)
LN2 = math.log(2.0)
WHOLE, FIRST, SECOND = 0, 1, 2
SLOT_DY = (0, 1, 3, 2)


RELAY, DIRECT, STRIDE = 0, 1, 2


def ring_sends(mode, offset, n):
    half = n // 2
    if mode == DIRECT:
        if offset:
            return []
        near = [(s * k, s * k % n, WHOLE) for k in range(1, half) for s in (1, -1)]
        return near + [(half, half, WHOLE)]
    if mode == STRIDE and n == 8:
        if offset == 0:
            return [(1, 1, WHOLE), (-1, 7, WHOLE), (2, 2, WHOLE), (-2, 6, WHOLE)]
        if offset == 2:
            return [(1, 3, WHOLE), (2, 4, FIRST)]
        if offset == 6:
            return [(-1, 5, WHOLE), (-2, 4, SECOND)]
        return []
    out = []
    if offset == 0 or offset < half:
        new = offset + 1
        if new <= half:
            out.append((1, new, WHOLE if new < half else FIRST))
    if offset == 0 or offset > half:
        new = (offset or n) - 1
        if new >= half:
            out.append((-1, new, WHOLE if new > half else SECOND))
    return out


def parts_in(mode, offset, n):
    return 2 if mode != DIRECT and offset == n // 2 else 1


X_FIRST, Z_SECOND, Z_FIRST, X_SECOND, Q_RING = DIRECT, RELAY, STRIDE, RELAY, DIRECT


def parts_of(key, nz, nx, ny):
    if key[0] == "q":
        return parts_in(Q_RING, key[1], ny)
    _, half, dz, dx = key
    if half == 0:
        return parts_in(X_FIRST, dx, nx) if dz == 0 else parts_in(Z_SECOND, dz, nz)
    return parts_in(Z_FIRST, dz, nz) if dx == 0 else parts_in(X_SECOND, dx, nx)


def sends_of(key, nz, nx, ny):
    if key[0] == "q":
        return [("y", s, ("q", new), p) for s, new, p in ring_sends(Q_RING, key[1], ny)]
    _, half, dz, dx = key
    modes = (X_FIRST, Z_SECOND) if half == 0 else (X_SECOND, Z_FIRST)
    along_x = [("x", s, ("kv", half, dz, new), p) for s, new, p in ring_sends(modes[0], dx, nx)]
    along_z = [("z", s, ("kv", half, new, dx), p) for s, new, p in ring_sends(modes[1], dz, nz)]
    if half == 0:
        return (along_x if dz == 0 else []) + along_z
    return (along_z if dx == 0 else []) + along_x


def planes_in_order(nz):
    order = [0]
    for d in range(1, nz // 2):
        order += [d, nz - d]
    return order + [nz // 2]


def compute_units(nz, nx):
    planes = planes_in_order(nz)
    pieces = lambda p: [("kv", h, p, dx) for h in (0, 1) for dx in range(nx)]
    need_q = [[("q", SLOT_DY[0]), ("q", SLOT_DY[1])], [("q", SLOT_DY[2]), ("q", SLOT_DY[3])]]
    units = [(("first", r, 0), pieces(0) + need_q[r], 0.5) for r in (0, 1)]
    for c in range((nz - 2) // 2):
        needs = pieces(planes[1 + 2 * c]) + pieces(planes[2 + 2 * c])
        units += [(("main", r, c), needs + need_q[r], 0.85) for r in (0, 1)]
    units += [(("last", slot, 0), pieces(nz // 2), 0.3) for slot in (3, 1, 2, 0)]
    return units


def plan(nz, nx, ny, latency=2.3, hop=0.75, rate=50000.0, issue=0.03):
    units = compute_units(nz, nx)
    busy, coming, took, done, steps, now = {}, [], {}, set(), [], 0.0
    counts = {"z": nz, "x": nx, "y": ny}

    def complete(key):
        done.add(key)
        size = 98304 if key[0] == "q" else (24576, 40960)[key[1]]
        for axis, step, new, part in sends_of(key, nz, nx, ny):
            time = (size if part == WHOLE else size // 2) / rate
            ways = (1, -1) if 2 * abs(step) == counts[axis] else (1 if step > 0 else -1,)
            end = 0.0
            for way in ways:
                busy[axis, way] = max(busy.get((axis, way), 0.0), now) + time * abs(step) / len(ways)
                end = max(end, busy[axis, way])
            heapq.heappush(coming, (end + latency + hop * (abs(step) - 1), new, part))

    for key in (("kv", 1, 0, 0), ("kv", 0, 0, 0), ("q", 0)):
        complete(key)
    while coming or units:
        if coming and coming[0][0] <= now:
            _, key, part = heapq.heappop(coming)
            now += issue
            steps.append(("take", key, part))
            took[key] = took.get(key, 0) + 1
            if took[key] == parts_of(key, nz, nx, ny):
                complete(key)
            continue
        ready, seen = [], set()
        for u in units:
            rows = u[0][1] // 2 if u[0][0] == "last" else u[0][1]
            if rows not in seen and all(d in done for d in u[1]):
                ready.append(u)
            seen.add(rows)
        if ready:
            units.remove(ready[0])
            now += ready[0][2]
            steps.append(ready[0][0])
            continue
        now = coming[0][0]
    return steps


def reached(nz, nx, ny):
    keys = [("kv", h, z, x) for h in (0, 1) for z in range(nz) for x in range(nx)]
    counts = {"z": nz, "x": nx, "y": ny}
    steps = {("y", k) for k in range(1, ny)}
    for key in keys + [("q", 0)]:
        for axis, step, _, _ in sends_of(key, nz, nx, ny):
            steps |= {(axis, step % counts[axis]), (axis, -step % counts[axis])}
    return sorted(steps)


def kernel(
    sizes,
    q_hbm, k_hbm, v_hbm, order_hbm, w_hbm,
    out_ref, lse_ref,
    order_ref, q_buf, kv, m_buf, acc, w_buf, w_other, own_o, own_st, o_send, st_send, o_recv, st_recv,
    att, att_recv,
    load_sem, kv_recv, q_recv, kv_send, q_send, o_send_sem, st_send_sem, o_recv_sem, st_recv_sem,
    swap_sem,
):
    nz, nx, ny = sizes
    tok = k_hbm.shape[0]
    cut = tok * 3 // 8
    width = out_ref.shape[1]
    head = lax.axis_index("head")
    pos = {a: lax.axis_index(AXIS[a]) for a in "zxy"}
    size = {"z": nz, "x": nx, "y": ny}

    def at(axis, delta):
        n = size[axis]
        return lax.rem(pos[axis] + (delta % n), n)

    def peer(axis, delta):
        return {AXIS[axis]: at(axis, delta)}

    def remote(src, dst, send, recv, to):
        return pltpu.make_async_remote_copy(
            src_ref=src, dst_ref=dst, send_sem=send, recv_sem=recv,
            device_id=to, device_id_type=pl.DeviceIdType.MESH,
        )

    loads = [(k_hbm, kv.at[0, 0]), (v_hbm, kv.at[0, 1])]
    for g in range(GROUP):
        loads.append((q_hbm.at[:, g * DH:(g + 1) * DH], q_buf.at[0, g]))
    loads.append((order_hbm, order_ref))
    for c in (0, 1):
        loads.append((w_hbm.at[:, c * width:(c + 1) * width], w_buf.at[c]))
    loads = [pltpu.make_async_copy(s, d, load_sem.at[i]) for i, (s, d) in enumerate(loads)]
    kv_loads, q_loads, w_loads = loads[:2], loads[2:6], loads[6:]
    for copy in kv_loads + q_loads:
        copy.start()

    barrier = pltpu.get_barrier_semaphore()
    partner = {"head": 1 - head}
    peers = [peer(*step) for step in reached(nz, nx, ny)] + [partner]
    for p in peers:
        pl.semaphore_signal(barrier, inc=1, device_id=p, device_id_type=pl.DeviceIdType.MESH)
    for copy in kv_loads:
        copy.wait()
    pl.semaphore_wait(barrier, len(peers))

    planes = planes_in_order(nz)
    place = {p: i for i, p in enumerate(planes)}

    def view(key, part):
        if key[0] == "q":
            return q_buf.at[SLOT_DY.index(key[1])]
        _, h, dz, dx = key
        rows = slice(0, cut) if h == 0 else slice(cut, tok)
        slot = place[dz] * nx + dx
        return kv.at[slot, :, rows] if part == WHOLE else kv.at[slot, part - 1, rows]

    def arrival_sem(key, part):
        if key[0] == "q":
            return q_recv.at[key[1]]
        _, h, dz, dx = key
        return kv_recv.at[((h * nz + dz) * nx + dx) * 2 + (1 if part == SECOND else 0)]

    def send_on(key):
        for axis, step, new, part in sends_of(key, nz, nx, ny):
            remote(
                view(key, part), view(new, part), q_send if key[0] == "q" else kv_send,
                arrival_sem(new, part), peer(axis, step),
            ).start()

    taken = {}

    def take(key, part):
        ref = view(key, part)
        pltpu.make_async_copy(ref, ref, arrival_sem(key, part)).wait()
        taken[key] = taken.get(key, 0) + 1
        if taken[key] == parts_of(key, nz, nx, ny):
            send_on(key)

    factor = DH ** (-0.5) * LOG2E

    def query_place(slot):
        return order_ref[(pos["z"] * nx + pos["x"]) * ny + at("y", -SLOT_DY[slot])]

    def key_place(plane, dx):
        return order_ref[(at("z", -plane) * nx + at("x", -dx)) * ny + pos["y"]]

    def bias_row(slot, chunk):
        mine = query_place(slot)
        parts = []
        for plane in chunk:
            for dx in range(nx):
                b = jnp.where(key_place(plane, dx) > mine, NEG, 0.0).astype(jnp.float32)
                parts.append(jnp.full((1, tok), b, jnp.float32))
        return jnp.concatenate(parts, axis=1)

    def rows_of(which, chunk):
        first = place[chunk[0]] * nx
        count = len(chunk) * nx
        return kv[first:first + count, which].reshape(count * tok, DH)

    def attend(slots, chunk, first):
        key_rows = rows_of(0, chunk)
        value_rows = rows_of(1, chunk)
        value_rows = jnp.concatenate([value_rows, jnp.ones_like(value_rows)], axis=1)
        for slot in slots:
            bias = bias_row(slot, chunk)
            if first and slot == 0:
                r = lax.broadcasted_iota(jnp.int32, (tok, tok), 0)
                c = lax.broadcasted_iota(jnp.int32, (tok, tok), 1)
                corner = jnp.where(c <= r, 0.0, NEG).astype(jnp.float32)
                rest = jnp.broadcast_to(bias[:, tok:], (tok, bias.shape[1] - tok))
                bias = jnp.concatenate([corner, rest], axis=1)
            for g in range(GROUP):
                scores = lax.dot_general(
                    q_buf[slot, g], key_rows, (((1,), (1,)), ((), ())),
                    preferred_element_type=jnp.float32,
                )
                scores = scores * factor + bias
                top = jnp.max(scores, axis=1, keepdims=True)
                if not first:
                    old = m_buf[slot, g]
                    new = jnp.maximum(old, top)
                    shrink = jnp.exp2(old - new)
                    top = new[:, :1]
                else:
                    new = jnp.broadcast_to(top, (tok, DH))
                weights = jnp.exp2(scores - top).astype(jnp.bfloat16)
                both = jnp.dot(weights, value_rows, preferred_element_type=jnp.float32)
                if not first:
                    both = both + acc[slot, g] * jnp.concatenate([shrink, shrink], axis=1)
                m_buf[slot, g] = new
                acc[slot, g] = both

    def finish(slot):
        row = lax.broadcasted_iota(jnp.int32, (8, tok), 0)
        stats = None
        for g in range(GROUP):
            both = acc[slot, g]
            total = both[:, DH:]
            o = both[:, :DH] / total
            flat = jnp.transpose(m_buf[slot, g] + jnp.log(total) * LOG2E)[:8]
            stats = flat if g == 0 else jnp.where(row < g, stats, flat)
            if slot == 0:
                own_o[g] = o
            else:
                o_send[slot, g] = o.astype(jnp.bfloat16)
        if slot == 0:
            own_st[...] = stats
        else:
            st_send[slot] = stats

    def back(slot):
        to = peer("y", -SLOT_DY[slot])
        return [
            remote(o_send.at[slot], o_recv.at[slot], o_send_sem.at[slot], o_recv_sem.at[slot], to),
            remote(st_send.at[slot], st_recv.at[slot], st_send_sem.at[slot], st_recv_sem.at[slot], to),
        ]

    send_on(("kv", 1, 0, 0))
    send_on(("kv", 0, 0, 0))
    for copy in q_loads:
        copy.wait()
    send_on(("q", 0))
    for copy in w_loads:
        copy.start()
    w_swap = remote(w_buf.at[1 - head], w_other, swap_sem.at[0], swap_sem.at[1], partner)

    sent = [w_swap]
    for step in plan(nz, nx, ny):
        if step[0] == "take":
            take(*step[1:])
            continue
        kind, which, c = step
        if kind == "first":
            attend((0, 1) if which == 0 else (2, 3), (0,), True)
            if which == 1:
                for copy in w_loads:
                    copy.wait()
                w_swap.start()
        elif kind == "main":
            attend((0, 1) if which == 0 else (2, 3), planes[1 + 2 * c:3 + 2 * c], False)
        else:
            attend((which,), (nz // 2,), False)
            finish(which)
            if which:
                copies = back(which)
                for copy in copies:
                    copy.start()
                sent += copies

    for slot in (1, 2, 3):
        pltpu.make_async_copy(st_recv.at[slot], st_recv.at[slot], st_recv_sem.at[slot]).wait()
    logs = [own_st[...]] + [st_recv[slot] for slot in (1, 2, 3)]
    top = functools.reduce(jnp.maximum, logs)
    parts = [jnp.exp2(a - top) for a in logs]
    total = functools.reduce(jnp.add, parts)
    lse_ref[...] = (top * LN2 + jnp.log(total))[:GROUP]
    shares = [p / total for p in parts]
    shares = jnp.concatenate(shares + [jnp.zeros((DH - 32, tok), jnp.float32)], axis=0)
    shares = jnp.transpose(shares)

    for slot in (1, 2, 3):
        pltpu.make_async_copy(o_recv.at[slot], o_recv.at[slot], o_recv_sem.at[slot]).wait()
    for g in range(GROUP):
        o = own_o[g] * shares[:, g:g + 1]
        for slot in (1, 2, 3):
            o = o + o_recv[slot, g].astype(jnp.float32) * shares[:, 8 * slot + g:8 * slot + g + 1]
        att[:, g * DH:(g + 1) * DH] = o.astype(jnp.bfloat16)
    swap = remote(att, att_recv, swap_sem.at[2], swap_sem.at[3], partner)
    swap.start()
    sent.append(swap)

    tile = width // 3
    attended = att[...]
    for j in range(0, width, tile):
        p = jnp.dot(attended, w_buf[head, :, j:j + tile], preferred_element_type=jnp.float32)
        out_ref[:, j:j + tile] = p.astype(jnp.bfloat16)
    w_swap.wait_recv()
    swap.wait_recv()
    attended = att_recv[...]
    for j in range(0, width, tile):
        p = jnp.dot(attended, w_other[:, j:j + tile], preferred_element_type=jnp.float32)
        p = p.astype(jnp.bfloat16).astype(jnp.float32)
        both = out_ref[:, j:j + tile].astype(jnp.float32) + p
        out_ref[:, j:j + tile] = both.astype(jnp.bfloat16)

    pltpu.make_async_copy(kv.at[1:], kv.at[1:], kv_send).wait()
    pltpu.make_async_copy(q_buf.at[1:], q_buf.at[1:], q_send).wait()
    for copy in sent:
        copy.wait_send()


def put_out(a_ref, b_ref, out_ref, lse_ref, sems):
    copies = [
        pltpu.make_async_copy(a_ref, out_ref, sems.at[0]),
        pltpu.make_async_copy(b_ref, lse_ref, sems.at[1]),
    ]
    for copy in copies:
        copy.start()
    for copy in copies:
        copy.wait()


def body(sizes, queries, keys, values, stretch_order, out_weight):
    nz, nx, ny = sizes
    tok = queries.shape[0]
    width = out_weight.shape[1] // 2
    bf, f32 = jnp.bfloat16, jnp.float32
    vmem = pl.BlockSpec(memory_space=pltpu.VMEM)
    hbm = pl.BlockSpec(memory_space=pltpu.HBM)
    dma = pltpu.SemaphoreType.DMA
    results = (
        jax.ShapeDtypeStruct((tok, width), bf),
        jax.ShapeDtypeStruct((GROUP, tok), f32),
    )
    call = pl.pallas_call(
        functools.partial(kernel, sizes),
        name="attend_and_project",
        out_shape=results,
        in_specs=[hbm] * 5,
        out_specs=(vmem, vmem),
        scratch_shapes=[
            pltpu.SMEM(stretch_order.shape, jnp.int32),
            pltpu.VMEM((ny, GROUP, tok, DH), bf),
            pltpu.VMEM((nz * nx, 2, tok, DH), bf),
            pltpu.VMEM((ny, GROUP, tok, DH), f32),
            pltpu.VMEM((ny, GROUP, tok, 2 * DH), f32),
            pltpu.VMEM((2, GROUP * DH, width), bf),
            pltpu.VMEM((GROUP * DH, width), bf),
            pltpu.VMEM((GROUP, tok, DH), f32),
            pltpu.VMEM((8, tok), f32),
            pltpu.VMEM((ny, GROUP, tok, DH), bf),
            pltpu.VMEM((ny, 8, tok), f32),
            pltpu.VMEM((ny, GROUP, tok, DH), bf),
            pltpu.VMEM((ny, 8, tok), f32),
            pltpu.VMEM((tok, GROUP * DH), bf),
            pltpu.VMEM((tok, GROUP * DH), bf),
            dma((8,)),
            dma((4 * nz * nx,)),
            dma((ny,)),
            dma,
            dma,
            dma((ny,)),
            dma((ny,)),
            dma((ny,)),
            dma((ny,)),
            dma((4,)),
        ],
        compiler_params=pltpu.CompilerParams(
            collective_id=0, has_side_effects=True, vmem_limit_bytes=32 * 1024 * 1024
        ),
    )
    args = (queries, keys, values, stretch_order, out_weight)
    mixed, logs = call(*(in_hbm(a) for a in args))
    return pl.pallas_call(
        put_out,
        name="put_out",
        out_shape=results,
        in_specs=[vmem, vmem],
        out_specs=(hbm, hbm),
        scratch_shapes=[dma((2,))],
        compiler_params=pltpu.CompilerParams(vmem_limit_bytes=4 * 1024 * 1024),
    )(mixed, logs)


def in_hbm(x):
    return pltpu.with_memory_space_constraint(x, pltpu.HBM)


def solution(mesh):
    nz, nx, ny = 8, 4, mesh.shape["rep"]
    split = Mesh(
        mesh.devices.reshape(mesh.shape["head"], nz, nx, ny),
        ("head", "blk_0", "blk_1", "rep"),
    )
    in_specs = (P(BLK_REP, "head"), P(BLK_REP, "head"), P(BLK_REP, "head"), P(), P("head", None))
    out_specs = (P(BLK_REP, "head"), P("head", BLK_REP))
    return jax.shard_map(
        functools.partial(body, (nz, nx, ny)),
        mesh=split, in_specs=in_specs, out_specs=out_specs, check_vma=False,
    )
```
